32 devices in a mesh: expert: 8 (over y, x, core), tensor: 4 (over z).
Axes of the slice: x: 2, y: 2, z: 4, core: 2. Of those that a mesh axis runs over, the one named last changes fastest.
Arguments:
- tokens: bfloat16 [1024, 2560], P('expert', 'tensor'), may hold values from -6 to 6
- slot: int32 [1024, 1], P('expert'), may hold values from 0 to 15; in each aligned block of 128 rows (0 to 127, 128 to 255, ...) at most 16 rows name the same one
- mask: int32 [1024], P('expert'), may hold values 0 or 1
- hot_group: int32 [1], replicated, may hold values from 0 to 7
- router_weight: bfloat16 [2560, 8], replicated, may hold values from -0.125 to 0.125
- exp_gate: bfloat16 [8, 2560, 4096], P('expert', None, 'tensor'), may hold values from -0.125 to 0.125
- exp_up: bfloat16 [8, 2560, 4096], P('expert', None, 'tensor'), may hold values from -0.125 to 0.125
- exp_down: bfloat16 [8, 4096, 2560], P('expert', 'tensor'), may hold values from -0.09375 to 0.09375
- sh_gate: bfloat16 [2560, 4096], P('expert', 'tensor'), may hold values from -0.125 to 0.125
- sh_up: bfloat16 [2560, 4096], P('expert', 'tensor'), may hold values from -0.125 to 0.125
- sh_down: bfloat16 [4096, 2560], P('tensor', 'expert'), may hold values from -0.09375 to 0.09375
Outputs:
- mixed: bfloat16 [1024, 2560], P('expert', 'tensor')
The draws below stay inside these ranges and needn't reach their ends.
Inputs may be any that keep to these rules, and one draw needn't show every extreme that they name: Slot 2 g is the home slot of expert g, slot 2 g + 1 the spare slot of group g. Among the 128 tokens of one group no slot is named by more than 16 tokens, a bound that some block reaches.
All inputs are finite; a program needn't handle non-finite values. No bound on the sum of `mask` on one device may be relied on, other than what follows from the above.
Results may differ from the reference program's by a relative error of at most 0.0052.
Values may be sent and summed in bfloat16 or wider, within the bound.
No kernel may reach another device: no remote copies, remote signals or barrier semaphores. Data moves between devices by JAX's collectives and lax.ppermute only.
A program may use at most 192 MiB of HBM per device.

```python
import math
import jax
import jax.numpy as jnp
import numpy as np
from jax import lax

D = 2560
FFE = 4096
FFS = 4096
TOK_DEV = 128
EXPERTS = 8
SLOTS = 16
CAP = 16
TOKENS = 1024
N_EXPERT = 8


def touch_ends(drawn, rng, least, largest):
    longest = drawn.shape.index(max(drawn.shape))
    spots = []
    for shift in (0, 1):
        where = [jax.random.randint(jax.random.fold_in(rng, axis), (), 0, length) for axis, length in enumerate(drawn.shape)]
        where[longest] = (where[longest] + shift) % drawn.shape[longest]
        spots.append(tuple(where))
    return drawn.at[spots[0]].set(least).at[spots[1]].set(largest)


def shard_levels(stream_key, dims, cuts, low, largest):
    def one(dim, parts):
        draws = jax.random.uniform(jax.random.fold_in(jax.random.fold_in(stream_key, 6), dim), (parts,), jnp.float32, low / len(cuts), largest / len(cuts))
        return jnp.repeat(jnp.exp(draws), dims[dim] // parts).reshape((-1,) + (1,) * (len(dims) - dim - 1))

    loudness = one(*cuts[0])
    for cut in cuts[1:]:
        loudness = loudness * one(*cut)
    return loudness


def shared_out(rng, own, number, rows, count, top, bound, lean):
    ranking = jax.random.permutation(rng, count)
    crowded, common = shares(count, rows * top, bound, lean, True), shares(count, rows * top, bound, lean, False)
    places = jnp.arange(count)

    def named(tallies, turn):
        used = int((tallies > 0).sum())
        fixed = max(1, used // 4)
        shifted = fixed + (places - fixed + turn * (used - fixed)) % max(1, count - fixed)
        return jnp.zeros((count,), jnp.int32).at[ranking[jnp.where(places < fixed, places, shifted)]].set(jnp.asarray(tallies, jnp.int32))

    tallies = jnp.where(number % 4 == 0, named(crowded, number // 4), named(common, number - number // 4 - 1))
    mixed = jax.random.permutation(jax.random.fold_in(own, 3), count)
    source_of, receiver = mixed[0:count // 2 * 2:2], mixed[1:count // 2 * 2:2]
    slack = jnp.minimum(tallies[source_of] - 1, bound - tallies[receiver]) // 2
    slack = jnp.where((source_of == ranking[0]) | (receiver == ranking[0]) | (tallies[receiver] == 0), 0, jnp.maximum(slack, 0))
    shifted = jax.random.randint(jax.random.fold_in(own, 4), (count // 2,), 0, 1 << 20) % (slack + 1)
    tallies = tallies.at[source_of].add(-shifted).at[receiver].add(shifted)
    items = jnp.searchsorted(jnp.cumsum(tallies), jnp.arange(rows * top), side="right").astype(jnp.int32)
    grid = items.reshape(top, rows).T
    grid = grid[jax.random.permutation(jax.random.fold_in(own, 1), rows)]
    turn = jax.random.randint(jax.random.fold_in(own, 2), (rows, 1), 0, top)
    return jnp.take_along_axis(grid, (jnp.arange(top)[None, :] + turn) % top, axis=1)


def shares(count, total, bound, lean, full):
    loads = [(1 << 20) // math.isqrt(rank ** lean) + 1 for rank in range(1, count + 1)]
    largest = bound if full else min(bound, max(-(-total // count), total * loads[0] // sum(loads)))
    least = 1 if total - largest >= count - 1 else 0
    given, surplus = [largest] + [least] * (count - 1), total - largest - least * (count - 1)
    while surplus > 0:
        candidates = [i for i in range(1, count) if given[i] < largest] or [i for i in range(1, count) if given[i] < bound]
        pool, budget = sum([loads[i] for i in candidates]), surplus
        for i in candidates:
            more = min(bound - given[i], max(1, budget * loads[i] // pool), surplus)
            given[i] = given[i] + more
            surplus = surplus - more
    return np.array(given)


def normal_values(rng, extent, deviation, bound, pieces=(), kind=jnp.bfloat16):
    factor_of = shard_levels(rng, extent, pieces, -0.22, 0.18) if pieces else 1.0
    array = jax.random.normal(rng, extent, jnp.float32) * deviation * factor_of
    return jnp.minimum(jnp.maximum(array, -bound), bound).astype(kind)


def setup_inputs(seed: int = 0) -> dict:
    splits = jax.random.split(jax.random.key(seed), 12)
    tokens = normal_values(splits[0], (TOKENS, D), 1.0, 6.0, ((0, 8), (1, 4)))
    slot_keys = jax.random.split(jax.random.fold_in(splits[1], 1), TOKENS // TOK_DEV)
    slot_turns = jax.random.permutation(jax.random.fold_in(splits[1], 3), TOKENS // TOK_DEV)
    slot = jax.vmap(lambda own, number: shared_out(jax.random.fold_in(splits[1], 2), own, number, TOK_DEV, SLOTS, 1, CAP, 2))(slot_keys, slot_turns).reshape((TOKENS, 1))
    mask = touch_ends((jax.random.randint(splits[2], (TOKENS,), 0, 8) < 7).astype(jnp.int32), jax.random.fold_in(splits[2], 1), 0, 1)
    hot_group = jax.random.randint(splits[3], (1,), 0, N_EXPERT).astype(jnp.int32)
    router_weight = normal_values(splits[4], (D, EXPERTS), D ** -0.5, 0.125)
    exp_gate = normal_values(splits[5], (EXPERTS, D, FFE), D ** -0.5, 0.125, ((0, 8), (2, 4)))
    exp_up = normal_values(splits[6], (EXPERTS, D, FFE), D ** -0.5, 0.125, ((0, 8), (2, 4)))
    exp_down = normal_values(splits[7], (EXPERTS, FFE, D), FFE ** -0.5, 0.09375, ((0, 8), (1, 4)))
    sh_gate = normal_values(splits[8], (D, FFS), D ** -0.5, 0.125, ((0, 8), (1, 4)))
    sh_up = normal_values(splits[9], (D, FFS), D ** -0.5, 0.125, ((0, 8), (1, 4)))
    sh_down = normal_values(splits[10], (FFS, D), FFS ** -0.5, 0.09375, ((0, 4), (1, 8)))
    return dict(tokens=tokens, slot=slot, mask=mask, hot_group=hot_group, router_weight=router_weight, exp_gate=exp_gate, exp_up=exp_up, exp_down=exp_down, sh_gate=sh_gate, sh_up=sh_up, sh_down=sh_down)


def expert_ffn(batch_rows, w_gate, w_up, w_down):
    gated = jnp.dot(batch_rows, w_gate, preferred_element_type=jnp.float32)
    upward = jnp.dot(batch_rows, w_up, preferred_element_type=jnp.float32)
    hidden = (jax.nn.silu(gated) * upward).astype(jnp.bfloat16)
    return jnp.dot(hidden, w_down, preferred_element_type=jnp.float32)


def reference(tokens, slot, mask, hot_group, router_weight, exp_gate, exp_up, exp_down, sh_gate, sh_up, sh_down):
    slot_ids = slot[:, 0].astype(jnp.int32)
    hot_index = hot_group[0].astype(jnp.int32)
    expert_id = jnp.where(slot_ids % 2 == 0, slot_ids // 2, hot_index).astype(jnp.int32)
    logits = jnp.dot(tokens, router_weight, preferred_element_type=jnp.float32)
    chosen = expert_id[:, None] == jnp.arange(EXPERTS, dtype=jnp.int32)[None, :]
    weighting = jax.nn.sigmoid(jnp.sum(jnp.where(chosen, logits, jnp.zeros_like(logits)), axis=1))
    shared = expert_ffn(tokens, sh_gate, sh_up, sh_down)
    rows_most = N_EXPERT * CAP
    ordering = jnp.argsort(slot_ids, stable=True).astype(jnp.int32)
    counts = jnp.sum((slot_ids[:, None] == jnp.arange(SLOTS, dtype=jnp.int32)[None, :]).astype(jnp.int32), axis=0).astype(jnp.int32)
    starts = (jnp.cumsum(counts) - counts).astype(jnp.int32)
    padded = jnp.concatenate([tokens[ordering], jnp.zeros((rows_most, D), tokens.dtype)], axis=0)

    def per_slot(slot_index):
        batch_rows = lax.dynamic_slice(padded, (starts[slot_index], jnp.int32(0)), (rows_most, D))
        which = jnp.where(slot_index % 2 == 0, slot_index // 2, hot_index).astype(jnp.int32)
        result = expert_ffn(batch_rows, exp_gate[which], exp_up[which], exp_down[which]).astype(jnp.bfloat16)
        within = jnp.arange(rows_most, dtype=jnp.int32) < counts[slot_index]
        return jnp.where(within[:, None], result, jnp.zeros_like(result))

    outputs = lax.map(per_slot, jnp.arange(SLOTS, dtype=jnp.int32))
    sorted_slots = slot_ids[ordering]
    offsets = (jnp.arange(TOKENS, dtype=jnp.int32) - starts[sorted_slots]).astype(jnp.int32)
    in_order = outputs[sorted_slots, offsets]
    routed = jnp.zeros_like(in_order).at[ordering].set(in_order)
    keep_rows = mask.astype(jnp.float32)
    mixed = keep_rows[:, None] * (shared + weighting[:, None] * routed.astype(jnp.float32))
    return mixed.astype(jnp.bfloat16)
```

```python
import jax
import jax.numpy as jnp
from jax import lax
from jax.sharding import PartitionSpec as P


def swap(block, bit):
    size = lax.axis_size("expert")
    return lax.ppermute(block, "expert", [(i, i ^ bit) for i in range(size)])


def orders(size):
    bits = [1 << k for k in range(1, size.bit_length() - 1)]
    turn = len(bits) // 2
    return bits, bits[turn:] + bits[:turn]


def spread(halves, n_groups):
    pieces = [{0: halves[0]}, {0: halves[1]}]
    mates = [{1: swap(halves[0], 1)}, {1: swap(halves[1], 1)}]
    routes = orders(n_groups)
    early = None
    for phase in range(len(routes[0])):
        if phase == len(routes[0]) - 1:
            early = [sorted(list(p) + list(m)) for p, m in zip(pieces, mates)]
        arrived = [{j | r[phase]: swap(b, r[phase]) for j, b in p.items()} for r, p in zip(routes, pieces)]
        for p, m, new in zip(pieces, mates, arrived):
            p.update(new)
            m.update({j | 1: swap(b, 1) for j, b in new.items()})
    for p, m in zip(pieces, mates):
        p.update(m)
    late = [sorted(set(p) - set(e)) for p, e in zip(pieces, early)]
    return pieces, early, late


def gather_up(partial, n_groups):
    routes = orders(n_groups)
    kept = []
    for p in partial:
        kept.append({j: p[j] + swap(p[j | 1], 1) for j in p if j & 1 == 0})
    for phase in reversed(range(len(routes[0]))):
        for r, acc in zip(routes, kept):
            bit = r[phase]
            for j in [j for j in acc if j & bit]:
                acc[j ^ bit] = acc[j ^ bit] + swap(acc.pop(j), bit)
    return [acc[0] for acc in kept]


def local(
    tokens,
    slot,
    mask,
    hot_group,
    router_weight,
    exp_gate,
    exp_up,
    exp_down,
    sh_gate,
    sh_up,
    sh_down,
):
    n_groups = lax.axis_size("expert")
    me = lax.axis_index("expert")
    f32, bf16 = jnp.float32, jnp.bfloat16
    my_gate = lax.all_to_all(sh_gate, "expert", 1, 0, tiled=True)
    my_up = lax.all_to_all(sh_up, "expert", 1, 0, tiled=True)
    my_down = lax.all_to_all(sh_down, "expert", 0, 1, tiled=True)
    whole = lax.all_gather(tokens, "tensor", axis=1, tiled=True)
    rows, width = whole.shape
    half = rows // 2
    ids = slot.reshape(1, rows)
    names = {0: ids}
    bit = 1
    while bit < n_groups:
        names.update({j | bit: swap(b, bit) for j, b in list(names.items())})
        bit *= 2
    pieces, early, late = spread([whole[:half], whole[half:]], n_groups)

    def ffn(keys):
        batch = jnp.concatenate([pieces[h][j] for h in (0, 1) for j in keys[h]], axis=0)
        slots = jnp.concatenate(
            [names[j][0, h * half : (h + 1) * half] for h in (0, 1) for j in keys[h]], axis=0
        )
        expert_id = jnp.where(slots % 2 == 0, slots // 2, hot_group[0])
        logits = jnp.dot(batch, router_weight, preferred_element_type=f32)
        column = lax.broadcasted_iota(jnp.int32, (1, router_weight.shape[1]), 1) == me
        weighting = jax.nn.sigmoid(jnp.sum(jnp.where(column, logits, 0.0), axis=1))
        weighting = jnp.where(expert_id == me, weighting, 0.0)
        gated = jnp.dot(batch, exp_gate[0], preferred_element_type=f32)
        upward = jnp.dot(batch, exp_up[0], preferred_element_type=f32)
        hidden = (jax.nn.silu(gated) * upward * weighting[:, None]).astype(bf16)
        sh_gated = jnp.dot(batch, my_gate, preferred_element_type=f32)
        sh_upward = jnp.dot(batch, my_up, preferred_element_type=f32)
        sh_hidden = (jax.nn.silu(sh_gated) * sh_upward).astype(bf16)
        total = jnp.dot(sh_hidden, my_down, preferred_element_type=f32)
        total = (total + jnp.dot(hidden, exp_down[0], preferred_element_type=f32)).astype(bf16)
        out, at = [{}, {}], 0
        for h in (0, 1):
            for j in keys[h]:
                out[h][j] = total[at : at + half]
                at += half
        return out

    first, second = ffn(early), ffn(late)
    partial = [{**a, **b} for a, b in zip(first, second)]
    mine = jnp.concatenate(gather_up(partial, n_groups), axis=0)
    n_cuts = lax.axis_size("tensor")
    sent = mine.reshape(rows, n_cuts, width // n_cuts).transpose(1, 0, 2)
    terms = lax.all_to_all(sent, "tensor", 0, 0, tiled=True)
    mixed = jnp.sum(terms.astype(f32), axis=0) * mask.astype(f32)[:, None]
    return mixed.astype(bf16)


def solution(mesh):
    in_specs = (
        P("expert", "tensor"),
        P("expert", None),
        P("expert"),
        P(),
        P(),
        P("expert", None, "tensor"),
        P("expert", None, "tensor"),
        P("expert", "tensor", None),
        P("expert", "tensor"),
        P("expert", "tensor"),
        P("tensor", "expert"),
    )
    out_specs = P("expert", "tensor")
    return jax.shard_map(local, mesh=mesh, in_specs=in_specs, out_specs=out_specs, check_vma=False)
```

```python
import functools

import jax
import jax.numpy as jnp
from jax import lax
from jax.experimental import pallas as pl
from jax.experimental.pallas import tpu as pltpu
from jax.sharding import PartitionSpec as P


F32, BF16 = jnp.float32, jnp.bfloat16
ROWS = 512
BLOCK = 512
ANY, VMEM = pl.BlockSpec(memory_space=pl.ANY), pl.BlockSpec(memory_space=pltpu.VMEM)


def swap(block, axis, bit):
    return lax.ppermute(block, axis, [(i, i ^ bit) for i in range(lax.axis_size(axis))])


def orders(size):
    bits = [1 << k for k in range(1, size.bit_length() - 1)]
    turn = len(bits) // 2
    return bits, bits[turn:] + bits[:turn]


def tie(*values):
    return lax.optimization_barrier(values)


def ffn_kernel(first, routed, n_pieces, n_strips, n_cuts, meta, *refs):
    pieces, refs = refs[:n_pieces], refs[n_pieces:]
    strips, refs = refs[:n_strips], refs[n_strips:]
    if routed:
        router, gate, up, down, *refs = refs
    elif n_strips:
        base, *refs = refs
    outs, refs = (refs[:2], refs[2:]) if n_strips else (refs[:1], refs[1:])
    if first:
        raw, (router, gate, up, down), refs = (router, gate, up, down), refs[:4], refs[4:]
        gu_sem, d_sem, *refs = refs
    x, x_sem, *refs = refs
    width = outs[0].shape[1]
    depth = width // n_cuts
    span = pieces[0].shape[0]
    loads = [pltpu.make_async_copy(p, x.at[pl.ds(i * span, span), :], x_sem.at[i]) for i, p in enumerate(pieces)]
    for copy in loads:
        copy.start()
    if first:
        units = gate.shape[2]
        spans = [pl.ds(at, min(BLOCK, units)) for at in range(0, units, min(BLOCK, units))]
        gu_loads = [
            [
                pltpu.make_async_copy(raw[1].at[:, :, lanes], gate.at[:, :, lanes], gu_sem.at[0, i]),
                pltpu.make_async_copy(raw[2].at[:, :, lanes], up.at[:, :, lanes], gu_sem.at[1, i]),
            ]
            for i, lanes in enumerate(spans)
        ]
        r_load = pltpu.make_async_copy(raw[0], router, d_sem.at[0])
        d_load = pltpu.make_async_copy(raw[3], down, d_sem.at[1])
        for copy in [r_load, *sum(gu_loads, []), d_load]:
            copy.start()
        r_load.wait()
    if n_strips:
        p_s, p_sem, *refs = refs
        strip, cols = strips[0].shape[0], strips[0].shape[1] // 3
        places = [pl.ds(pl.multiple_of(meta[2 + j], 16), strip) for j in range(n_strips)]
        p_loads = [pltpu.make_async_copy(s, p_s.at[places[j], :], p_sem.at[j]) for j, s in enumerate(strips)]
        for copy in p_loads:
            copy.start()
    for copy in loads:
        copy.wait()
    batch = x[:, :width]
    if routed:
        (h_s,) = refs
        units = gate.shape[2]
        slots = x[:, width : width + 1].astype(F32)
        home = jnp.floor(slots * 0.5)
        mine, hot = meta[0].astype(F32), meta[1].astype(F32)
        chosen = jnp.where(slots == 2.0 * home, home, hot) == mine
        logits = lax.dot_general(batch, router[...], (((1,), (1,)), ((), ())), preferred_element_type=F32)
        column = lax.broadcasted_iota(jnp.int32, logits.shape, 1) == meta[0]
        logit = jnp.sum(jnp.where(column, logits, 0.0), axis=1, keepdims=True)
        weighting = jnp.where(chosen, 1.0 / (1.0 + jnp.exp(-logit)), 0.0)
        block = min(BLOCK, units)
        for at in range(0, units, block):
            if first:
                for copy in gu_loads[at // block]:
                    copy.wait()
            lanes = slice(at, at + block)
            gated = jnp.dot(batch, gate[0, :, lanes], preferred_element_type=F32)
            upward = jnp.dot(batch, up[0, :, lanes], preferred_element_type=F32)
            h_s[:, lanes] = (gated / (1.0 + jnp.exp(-gated)) * upward * weighting).astype(BF16)
    if n_strips:
        for copy in p_loads:
            copy.wait()
        both = jnp.dot(batch, p_s[:, : 2 * cols], preferred_element_type=F32)
        gated = both[:, :cols]
        shared = (gated / (1.0 + jnp.exp(-gated)) * both[:, cols:]).astype(BF16)
    if first:
        d_load.wait()
    for k in range(n_cuts):
        here = slice(k * depth, (k + 1) * depth)
        if routed:
            total = jnp.dot(h_s[...], down[0, :, here], preferred_element_type=F32)
        else:
            total = base[:, here]
        if not n_strips:
            outs[0][:, here] = total
            continue
        sh_down = jnp.transpose(p_s[here, 2 * cols :], (1, 0))
        total = total + jnp.dot(shared, sh_down, preferred_element_type=F32)
        n_kept = outs[0].shape[0]
        outs[0][:, here] = total[:n_kept]
        outs[1][:, here] = total[n_kept:].astype(BF16)


def ffn(meta, pieces, strips, weights, base, n_cuts, first=False):
    routed = base is None
    n_pieces, n_strips = len(pieces), len(strips)
    rows, across = n_pieces * pieces[0].shape[0], pieces[0].shape[1]
    width, units = weights[1].shape[1:]
    dma = pltpu.SemaphoreType.DMA
    scratch = [pltpu.VMEM((rows, across), BF16), dma((n_pieces,))]
    outs = [pltpu.VMEM((rows, width), F32)]
    work = 0
    if n_strips:
        cols = strips[0].shape[1] // 3
        scratch += [pltpu.VMEM((width, 3 * cols), BF16), dma((n_strips,))]
        outs = [pltpu.VMEM((rows // 2, width), F32), pltpu.VMEM((rows // 2, width), BF16)]
        work += cols
    if routed:
        scratch += [pltpu.VMEM((rows, units), BF16)]
        work += units
    extra = list(weights) if routed else [base]
    if first:
        outs += [pltpu.VMEM(w.shape, BF16) for w in weights]
        scratch = [dma((2, max(1, units // BLOCK))), dma((2,))] + scratch
    out = pl.pallas_call(
        functools.partial(ffn_kernel, first, routed, n_pieces, n_strips, n_cuts),
        out_shape=tuple(outs),
        in_specs=[pl.BlockSpec(memory_space=pltpu.SMEM)] + [ANY] * (n_pieces + n_strips) + [ANY if first else VMEM] * len(extra),
        out_specs=(VMEM,) * len(outs),
        scratch_shapes=scratch,
        compiler_params=pltpu.CompilerParams(vmem_limit_bytes=16 * 1024 * 1024),
        cost_estimate=pl.CostEstimate(
            flops=6 * rows * width * work, bytes_accessed=6 * width * work, transcendentals=2 * rows * work
        ),
    )(meta, *pieces, *strips, *extra)
    return out if n_strips or first else out[0]


def local(
    tokens,
    slot,
    mask,
    hot_group,
    router_weight,
    exp_gate,
    exp_up,
    exp_down,
    sh_gate,
    sh_up,
    sh_down,
):
    n_groups, n_cuts = lax.axis_size("expert"), lax.axis_size("tensor")
    me, cut = lax.axis_index("expert"), lax.axis_index("tensor")
    rows, depth = tokens.shape
    half = rows // 2
    strip, cols = sh_gate.shape[0], sh_gate.shape[1] // n_groups
    numbers = [me, hot_group[0]] + [(me ^ j) * strip for j in range(n_groups)]
    meta = jnp.stack(numbers).astype(jnp.int32)

    features = [tokens] + [swap(tokens, "tensor", k) for k in range(1, n_cuts)]
    names = jnp.broadcast_to(slot.astype(BF16), (rows, 128))

    packed = jnp.concatenate(
        [
            sh_gate.reshape(strip, n_groups, cols).transpose(1, 0, 2),
            sh_up.reshape(strip, n_groups, cols).transpose(1, 0, 2),
            sh_down.reshape(n_groups, cols, strip).transpose(0, 2, 1),
        ],
        axis=2,
    )
    blocks = [lax.dynamic_index_in_dim(packed, me ^ j, 0, keepdims=False) for j in range(n_groups)]
    later = n_groups - max(1, n_groups // 4)
    strips = [blocks[0]] + [swap(blocks[j], "expert", j) for j in range(1, later)]
    weights = (router_weight.T, exp_gate, exp_up, exp_down)

    features, names, meta, _ = tie(features, names, meta, blocks)
    whole = jnp.concatenate([jnp.zeros((rows, depth * n_cuts), BF16), names], axis=1)
    for k, feature in enumerate(features):
        whole = lax.dynamic_update_slice(whole, feature, (0, (cut ^ k) * depth))
    halves = [whole[:half], whole[half:]]
    routes = orders(n_groups)
    last = len(routes[0]) - 1
    pieces = [{0: piece} for piece in halves]
    mates = [{1: swap(piece, "expert", 1)} for piece in halves]
    early = late = None
    for phase in range(last + 1):
        if phase == last:
            early = [{**p, **m} for p, m in zip(pieces, mates)]
            rest, _ = tie(blocks[later:], [list(p.values()) for p in pieces])
        arrived = [{j | r[phase]: swap(b, "expert", r[phase]) for j, b in p.items()} for r, p in zip(routes, pieces)]
        for p, m, new in zip(pieces, mates, arrived):
            p.update(new)
            m.update({j | 1: swap(b, "expert", 1) for j, b in new.items()})
        if phase == last:
            late = [{**new, **{j | 1: m[j | 1] for j in new}} for m, new in zip(mates, arrived)]
    strips += [swap(block, "expert", later + i) for i, block in enumerate(rest)]

    def batches(parts):
        even = [(h, j) for h in (0, 1) for j in sorted(parts[h]) if j & 1 == 0]
        many = min(len(even), ROWS // (2 * half))
        for at in range(0, len(even), many):
            stay = even[at : at + many]
            yield stay, [parts[h][j] for h, j in stay] + [parts[h][j | 1] for h, j in stay]

    acc = [{}, {}]

    def settle(stay, kept, sent):
        total = kept + swap(sent, "expert", 1).astype(F32)
        for i, (h, j) in enumerate(stay):
            acc[h][j] = total[i * half : (i + 1) * half]

    begun = []
    for stay, batch in batches(early):
        if begun:
            base = ffn(meta, batch, [], weights, None, n_cuts)
        else:
            base, *weights = ffn(meta, batch, [], weights, None, n_cuts, first=True)
        begun.append((stay, batch, base))
    meta, _ = tie(meta, [base for _, _, base in begun])
    for stay, batch in batches(late):
        kept, sent = ffn(meta, batch, strips, weights, None, n_cuts)
        settle(stay, kept, sent)
    meta, _ = tie(meta, kept)
    for stay, batch, base in begun:
        kept, sent = ffn(meta, batch, strips, weights, base, n_cuts)
        settle(stay, kept, sent)

    for phase in reversed(range(last + 1)):
        away = [[j for j in a if j & r[phase]] for r, a in zip(routes, acc)]
        sends = tie(*[jnp.concatenate([a.pop(j) for j in js], axis=0).astype(BF16) for a, js in zip(acc, away)])
        came = tie(*[swap(send, "expert", r[phase]) for r, send in zip(routes, sends)])
        for r, a, js, c in zip(routes, acc, away, came):
            for i, j in enumerate(js):
                a[j ^ r[phase]] = a[j ^ r[phase]] + c[i * half : (i + 1) * half].astype(F32)
    mine = jnp.concatenate([acc[0][0], acc[1][0]], axis=0)
    parts = [lax.dynamic_slice(mine, (0, (cut ^ k) * depth), (rows, depth)) for k in range(n_cuts)]
    sends = tie(*[part.astype(BF16) for part in parts[1:]])
    mixed = parts[0]
    for k, send in enumerate(sends):
        mixed = mixed + swap(send, "tensor", k + 1).astype(F32)
    return (mixed * mask.astype(F32)[:, None]).astype(BF16)


def solution(mesh):
    in_specs = (
        P("expert", "tensor"),
        P("expert", None),
        P("expert"),
        P(),
        P(),
        P("expert", None, "tensor"),
        P("expert", None, "tensor"),
        P("expert", "tensor", None),
        P("expert", "tensor"),
        P("expert", "tensor"),
        P("tensor", "expert"),
    )
    out_specs = P("expert", "tensor")
    return jax.shard_map(local, mesh=mesh, in_specs=in_specs, out_specs=out_specs, check_vma=False)
```

```python
import functools

import jax
import jax.numpy as jnp
from jax import lax
from jax.experimental import pallas as pl
from jax.experimental.pallas import tpu as pltpu
from jax.sharding import PartitionSpec as P


F32, BF16 = jnp.float32, jnp.bfloat16
ROWS = 512
BLOCK = 512
ANY, VMEM = pl.BlockSpec(memory_space=pl.ANY), pl.BlockSpec(memory_space=pltpu.VMEM)
HBM, SMEM = pl.BlockSpec(memory_space=pltpu.HBM), pl.BlockSpec(memory_space=pltpu.SMEM)
DMA = pltpu.SemaphoreType.DMA
MIB = 1024 * 1024


def swap(block, axis, bit):
    return lax.ppermute(block, axis, [(i, i ^ bit) for i in range(lax.axis_size(axis))])


def tie(*values):
    return lax.optimization_barrier(values)


def orders(size):
    bits = [1 << k for k in range(1, size.bit_length() - 1)]
    turn = len(bits) // 2
    return bits, bits[turn:] + bits[:turn]


def silu(v):
    return v / (1.0 + jnp.exp(-v))


def cost(flops, bytes_accessed):
    return pl.CostEstimate(flops=flops, bytes_accessed=bytes_accessed, transcendentals=0)


def stage_kernel(*refs):
    n = len(refs) // 2
    sources, targets, sems = refs[:n], refs[n : 2 * n], refs[2 * n]
    copies = [pltpu.make_async_copy(s, t, sems.at[i]) for i, (s, t) in enumerate(zip(sources, targets))]
    for copy in copies:
        copy.start()
    for copy in copies:
        copy.wait()


def stage(weights):
    return pl.pallas_call(
        stage_kernel,
        out_shape=tuple(pltpu.VMEM(w.shape, BF16) for w in weights),
        in_specs=[HBM] * len(weights),
        out_specs=(VMEM,) * len(weights),
        scratch_shapes=[DMA((len(weights),))],
        compiler_params=pltpu.CompilerParams(vmem_limit_bytes=42 * MIB),
        cost_estimate=cost(5 * 10**9, 2 * sum(w.size for w in weights)),
        name="stage",
    )(*weights)


def hidden_kernel(n_pieces, meta, *refs):
    pieces, (router, gate, up, hidden, x, sem) = refs[:n_pieces], refs[n_pieces:]
    width, units = gate.shape[1:]
    span = pieces[0].shape[0]
    loads = [pltpu.make_async_copy(p, x.at[pl.ds(i * span, span), :], sem.at[i]) for i, p in enumerate(pieces)]
    for copy in loads:
        copy.start()
    for copy in loads:
        copy.wait()
    batch = x[:, :width]
    slots = x[:, width : width + 1].astype(F32)
    home = jnp.floor(slots * 0.5)
    chosen = jnp.where(slots == 2.0 * home, home, meta[1].astype(F32)) == meta[0].astype(F32)
    logits = lax.dot_general(batch, router[...], (((1,), (1,)), ((), ())), preferred_element_type=F32)
    column = lax.broadcasted_iota(jnp.int32, logits.shape, 1) == meta[0]
    logit = jnp.sum(jnp.where(column, logits, 0.0), axis=1, keepdims=True)
    weighting = jnp.where(chosen, 1.0 / (1.0 + jnp.exp(-logit)), 0.0)
    block = min(BLOCK, units)
    for at in range(0, units, block):
        lanes = slice(at, at + block)
        gated = jnp.dot(batch, gate[0, :, lanes], preferred_element_type=F32)
        upward = jnp.dot(batch, up[0, :, lanes], preferred_element_type=F32)
        hidden[:, lanes] = (silu(gated) * upward * weighting).astype(BF16)


def routed_hidden(meta, pieces, weights):
    n_pieces = len(pieces)
    rows, across = n_pieces * pieces[0].shape[0], pieces[0].shape[1]
    width, units = weights[1].shape[1:]
    return pl.pallas_call(
        functools.partial(hidden_kernel, n_pieces),
        out_shape=(pltpu.VMEM((rows, units), BF16), pltpu.VMEM((rows, across), BF16)),
        in_specs=[SMEM] + [ANY] * n_pieces + [VMEM] * 3,
        out_specs=(VMEM, VMEM),
        scratch_shapes=[DMA((n_pieces,))],
        compiler_params=pltpu.CompilerParams(vmem_limit_bytes=10 * MIB),
        cost_estimate=cost(4 * rows * width * units, 4 * width * units),
        name="routed_hidden",
    )(meta, *pieces, *weights[:3])


def down_kernel(n_strips, n_cuts, meta, x, hidden, down, *refs):
    if n_strips:
        strips, refs = refs[:n_strips], refs[n_strips:]
        *outs, p_s, turned, sem = refs
    else:
        p_s, turned, *outs = refs
    width = down.shape[2]
    depth = width // n_cuts
    cols = turned.shape[1]
    places = [pl.ds(pl.multiple_of(meta[2 + k], 128), depth) for k in range(n_cuts)]
    if n_strips:
        strip = strips[0].shape[0]
        rows_of = [pl.ds(pl.multiple_of(meta[2 + n_cuts + j], 16), strip) for j in range(n_strips)]
        loads = [pltpu.make_async_copy(s, p_s.at[rows_of[j], :], sem.at[j]) for j, s in enumerate(strips)]
        for copy in loads:
            copy.start()
        for copy in loads:
            copy.wait()
    both = jnp.dot(x[:, :width], p_s[:, : 2 * cols], preferred_element_type=F32)
    shared = (silu(both[:, :cols]) * both[:, cols:]).astype(BF16)
    n_kept = x.shape[0] // 2
    for k in range(n_cuts):
        if n_strips:
            turned[k] = jnp.transpose(p_s[places[k], 2 * cols :], (1, 0))
        total = jnp.dot(hidden[...], down[0, :, places[k]], preferred_element_type=F32)
        total = total + jnp.dot(shared, turned[k], preferred_element_type=F32)
        kept, sent = outs[2 * (2 * k // n_cuts) : 2 * (2 * k // n_cuts) + 2]
        at = (k % (n_cuts // 2)) * depth
        kept[:, at : at + depth] = total[:n_kept]
        sent[:, at : at + depth] = total[n_kept:].astype(BF16)


def both_down(meta, x, hidden, down, strips, ready, n_cuts):
    rows, width = x.shape[0], down.shape[2]
    if ready:
        cols = ready[1].shape[1]
        extra, more, scratch = list(ready), [], []
    else:
        cols = strips[0].shape[1] // 3
        extra, scratch = list(strips), [DMA((len(strips),))]
        more = [pltpu.VMEM((width, 3 * cols), BF16), pltpu.VMEM((n_cuts, cols, width // n_cuts), BF16)]
    outs = [pltpu.VMEM((rows // 2, width // 2), F32), pltpu.VMEM((rows // 2, width // 2), BF16)] * 2 + more
    units = hidden.shape[1]
    out = pl.pallas_call(
        functools.partial(down_kernel, 0 if ready else len(strips), n_cuts),
        out_shape=tuple(outs),
        in_specs=[SMEM, VMEM, VMEM, VMEM] + [VMEM if ready else ANY] * len(extra),
        out_specs=(VMEM,) * len(outs),
        scratch_shapes=scratch,
        compiler_params=pltpu.CompilerParams(vmem_limit_bytes=8 * MIB),
        cost_estimate=cost(2 * rows * width * (units + 6 * cols), 2 * width * (units + 3 * cols)),
        name="both_down",
    )(meta, x, hidden, down, *extra)
    return [out[0:2], out[2:4]], ready or out[4:6]


def local(
    tokens,
    slot,
    mask,
    hot_group,
    router_weight,
    exp_gate,
    exp_up,
    exp_down,
    sh_gate,
    sh_up,
    sh_down,
):
    n_groups, n_cuts = lax.axis_size("expert"), lax.axis_size("tensor")
    me, cut = lax.axis_index("expert"), lax.axis_index("tensor")
    rows, depth = tokens.shape
    half = rows // 2
    strip, cols = sh_gate.shape[0], sh_gate.shape[1] // n_groups
    relative = list(reversed(range(n_cuts)))
    numbers = [me, hot_group[0]] + [(cut ^ k) * depth for k in relative] + [(me ^ j) * strip for j in range(n_groups)]
    meta = jnp.stack(numbers).astype(jnp.int32)

    features = [tokens] + [swap(tokens, "tensor", k) for k in range(1, n_cuts)]
    names = jnp.broadcast_to(slot.astype(BF16), (rows, 128))
    real = mask.astype(F32)[:, None]

    packed = jnp.concatenate(
        [
            sh_gate.reshape(strip, n_groups, cols).transpose(1, 0, 2),
            sh_up.reshape(strip, n_groups, cols).transpose(1, 0, 2),
            sh_down.reshape(n_groups, cols, strip).transpose(0, 2, 1),
        ],
        axis=2,
    )
    blocks = [lax.dynamic_index_in_dim(packed, me ^ j, 0, keepdims=False) for j in range(n_groups)]
    near_first = sorted(range(1, n_groups), key=lambda j: (j.bit_count(), j))
    soon, rest = near_first[: n_groups // 2 - 1], near_first[n_groups // 2 - 1 :]
    strips = {0: blocks[0]}
    strips.update({j: swap(blocks[j], "expert", j) for j in soon})

    features, names, real, meta, _ = tie(features, names, real, meta, blocks)
    whole = jnp.concatenate([jnp.zeros((rows, depth * n_cuts), BF16), names], axis=1)
    for k, feature in enumerate(features):
        whole = lax.dynamic_update_slice(whole, feature, (0, (cut ^ k) * depth))
    halves = [whole[:half], whole[half:]]
    weights = stage((router_weight.T, exp_gate, exp_up, exp_down))

    routes = orders(n_groups)
    last = len(routes[0]) - 1
    pieces = [{0: piece} for piece in halves]
    mates = [{1: swap(piece, "expert", 1)} for piece in halves]
    early = late = None
    for phase in range(last + 1):
        if phase == last:
            early = [{**p, **m} for p, m in zip(pieces, mates)]
        arrived = [
            {j | r[phase]: swap(b, "expert", r[phase]) for j, b in p.items() if j or phase < last}
            for r, p in zip(routes, pieces)
        ]
        if phase == last:
            arrived = [{r[phase]: swap(p[0], "expert", r[phase]), **new} for r, p, new in zip(routes, pieces, arrived)]
        for p, m, new in zip(pieces, mates, arrived):
            p.update(new)
            m.update({j | 1: swap(b, "expert", 1) for j, b in new.items()})
        if phase == last:
            late = [{**new, **{j | 1: m[j | 1] for j in new}} for m, new in zip(mates, arrived)]
    middle = len(rest) // 2
    for some in (rest[:middle], rest[middle:]):
        strips.update({j: swap(blocks[j], "expert", j) for j in some})
    strips = [strips[j] for j in range(n_groups)]

    def batches(parts):
        even = [(h, j) for h in (0, 1) for j in sorted(parts[h]) if j & 1 == 0]
        many = min(len(even), ROWS // (2 * half))
        for at in range(0, len(even), many):
            stay = even[at : at + many]
            yield stay, [parts[h][j] for h, j in stay] + [parts[h][j | 1] for h, j in stay]

    first, second, ready = [], [], None
    for stay, batch in batches(early):
        first.append((stay, routed_hidden(meta, batch, weights)))
    meta, _ = tie(meta, [done[0] for _, done in first])
    for stay, batch in batches(late):
        second.append((stay, routed_hidden(meta, batch, weights)))

    acc = [[{}, {}], [{}, {}]]

    def settle(stay, parts):
        for c, (kept, sent) in enumerate(parts):
            total = kept + swap(sent, "expert", 1).astype(F32)
            for i, (h, j) in enumerate(stay):
                acc[c][h][j] = total[i * half : (i + 1) * half]

    for stay, (hidden, x) in second:
        parts, ready = both_down(meta, x, hidden, weights[3], strips, ready, n_cuts)
        settle(stay, parts)
    for stay, (hidden, x) in first:
        parts, _ = both_down(meta, x, hidden, weights[3], strips, ready, n_cuts)
        settle(stay, parts)

    for phase in reversed(range(last + 1)):
        for c in (0, 1):
            away = [[j for j in a if j & r[phase]] for r, a in zip(routes, acc[c])]
            sends = [jnp.concatenate([a.pop(j) for j in js], axis=0).astype(BF16) for a, js in zip(acc[c], away)]
            came = tie(*[swap(send, "expert", r[phase]) for r, send in zip(routes, tie(*sends))])
            for r, a, js, got in zip(routes, acc[c], away, came):
                for i, j in enumerate(js):
                    a[j ^ r[phase]] = a[j ^ r[phase]] + got[i * half : (i + 1) * half].astype(F32)
    mixed = None
    for c in (0, 1):
        mine = jnp.concatenate([a[0] for a in acc[c]], axis=0)
        for i, k in enumerate(relative[c * n_cuts // 2 : (c + 1) * n_cuts // 2]):
            part = mine[:, i * depth : (i + 1) * depth]
            if k:
                part = swap(part.astype(BF16), "tensor", k).astype(F32)
            mixed = part if mixed is None else mixed + part
    return (mixed * real).astype(BF16)


def solution(mesh):
    in_specs = (
        P("expert", "tensor"),
        P("expert", None),
        P("expert"),
        P(),
        P(),
        P("expert", None, "tensor"),
        P("expert", None, "tensor"),
        P("expert", "tensor", None),
        P("expert", "tensor"),
        P("expert", "tensor"),
        P("tensor", "expert"),
    )
    out_specs = P("expert", "tensor")
    return jax.shard_map(local, mesh=mesh, in_specs=in_specs, out_specs=out_specs, check_vma=False)
```

```python
import functools

import jax
import jax.numpy as jnp
from jax import lax
from jax.experimental import pallas as pl
from jax.experimental.pallas import tpu as pltpu
from jax.sharding import PartitionSpec as P


F32, BF16 = jnp.float32, jnp.bfloat16
ROWS = 256
BLOCK = 512
ANY, VMEM = pl.BlockSpec(memory_space=pl.ANY), pl.BlockSpec(memory_space=pltpu.VMEM)
HBM, SMEM = pl.BlockSpec(memory_space=pltpu.HBM), pl.BlockSpec(memory_space=pltpu.SMEM)
DMA = pltpu.SemaphoreType.DMA
MIB = 1024 * 1024


def swap(block, axis, bit):
    return lax.ppermute(block, axis, [(i, i ^ bit) for i in range(lax.axis_size(axis))])


def tie(*values):
    return lax.optimization_barrier(values)


def orders(size):
    bits = [1 << k for k in range(1, size.bit_length() - 1)]
    turn = len(bits) // 2
    return bits, bits[turn:] + bits[:turn]


def silu(v):
    return v / (1.0 + jnp.exp(-v))


def cost(flops, bytes_accessed):
    return pl.CostEstimate(flops=flops, bytes_accessed=bytes_accessed, transcendentals=0)


def assemble_kernel(n_cuts, meta, *refs):
    features, names, outs = refs[:n_cuts], refs[n_cuts], refs[n_cuts + 1 :]
    depth = features[0].shape[1]
    half = outs[0].shape[0]
    for h, out in enumerate(outs):
        rows = slice(h * half, (h + 1) * half)
        out[:, n_cuts * depth :] = names[rows]
        for k, feature in enumerate(features):
            out[:, pl.ds(pl.multiple_of(meta[1 + n_cuts - k], 128), depth)] = feature[rows]


def assemble(meta, features, names):
    n_cuts, (rows, depth) = len(features), features[0].shape
    out = pltpu.VMEM((rows // 2, n_cuts * depth + names.shape[1]), BF16)
    return pl.pallas_call(
        functools.partial(assemble_kernel, n_cuts),
        out_shape=(out, out),
        in_specs=[SMEM] + [VMEM] * (n_cuts + 1),
        out_specs=(VMEM, VMEM),
        compiler_params=pltpu.CompilerParams(vmem_limit_bytes=2 * MIB),
        cost_estimate=cost(10**6, 4 * n_cuts * rows * depth),
        name="assemble",
    )(meta, *features, names)


def stage_kernel(*refs):
    n = len(refs) // 2
    sources, targets, sems = refs[:n], refs[n : 2 * n], refs[2 * n]
    copies = [pltpu.make_async_copy(s, t, sems.at[i]) for i, (s, t) in enumerate(zip(sources, targets))]
    for copy in copies:
        copy.start()
    for copy in copies:
        copy.wait()


def stage(weights):
    return pl.pallas_call(
        stage_kernel,
        out_shape=tuple(pltpu.VMEM(w.shape, BF16) for w in weights),
        in_specs=[HBM] * len(weights),
        out_specs=(VMEM,) * len(weights),
        scratch_shapes=[DMA((len(weights),))],
        compiler_params=pltpu.CompilerParams(vmem_limit_bytes=42 * MIB),
        cost_estimate=cost(5 * 10**9, 2 * sum(w.size for w in weights)),
        name="stage",
    )(*weights)


def hidden_kernel(n_pieces, meta, *refs):
    pieces, (router, gate, up, hidden, x) = refs[:n_pieces], refs[n_pieces:]
    width, units = gate.shape[1:]
    span = pieces[0].shape[0]
    for i, piece in enumerate(pieces):
        x[i * span : (i + 1) * span, :] = piece[...]
    batch = x[:, :width]
    slots = x[:, width : width + 1].astype(F32)
    home = jnp.floor(slots * 0.5)
    chosen = jnp.where(slots == 2.0 * home, home, meta[1].astype(F32)) == meta[0].astype(F32)
    logits = lax.dot_general(batch, router[...], (((1,), (1,)), ((), ())), preferred_element_type=F32)
    column = lax.broadcasted_iota(jnp.int32, logits.shape, 1) == meta[0]
    logit = jnp.sum(jnp.where(column, logits, 0.0), axis=1, keepdims=True)
    weighting = jnp.where(chosen, 1.0 / (1.0 + jnp.exp(-logit)), 0.0)
    block = min(BLOCK, units)
    for at in range(0, units, block):
        lanes = slice(at, at + block)
        gated = jnp.dot(batch, gate[0, :, lanes], preferred_element_type=F32)
        upward = jnp.dot(batch, up[0, :, lanes], preferred_element_type=F32)
        hidden[:, lanes] = (silu(gated) * upward * weighting).astype(BF16)


def routed_hidden(meta, pieces, weights):
    n_pieces = len(pieces)
    rows, across = n_pieces * pieces[0].shape[0], pieces[0].shape[1]
    width, units = weights[1].shape[1:]
    return pl.pallas_call(
        functools.partial(hidden_kernel, n_pieces),
        out_shape=(pltpu.VMEM((rows, units), BF16), pltpu.VMEM((rows, across), BF16)),
        in_specs=[SMEM] + [VMEM] * (n_pieces + 3),
        out_specs=(VMEM, VMEM),
        compiler_params=pltpu.CompilerParams(vmem_limit_bytes=10 * MIB),
        cost_estimate=cost(4 * rows * width * units, 4 * width * units),
        name="routed_hidden",
    )(meta, *pieces, *weights[:3])


def shared_units(p_s, batches, hiddens):
    cols = p_s.shape[1] // 3
    for batch, hidden in zip(batches, hiddens):
        both = jnp.dot(batch[:, : p_s.shape[0]], p_s[:, : 2 * cols], preferred_element_type=F32)
        hidden[...] = (silu(both[:, :cols]) * both[:, cols:]).astype(BF16)


def more_kernel(n_batches, p_s, *refs):
    shared_units(p_s, refs[:n_batches], refs[n_batches:])


def more_hidden(packed, batches):
    rows, (width, cols) = batches[0].shape[0], packed.shape
    return pl.pallas_call(
        functools.partial(more_kernel, len(batches)),
        out_shape=(pltpu.VMEM((rows, cols // 3), BF16),) * len(batches),
        in_specs=[VMEM] * (1 + len(batches)),
        out_specs=(VMEM,) * len(batches),
        compiler_params=pltpu.CompilerParams(vmem_limit_bytes=6 * MIB),
        cost_estimate=cost(2 * rows * width * cols * len(batches), 2 * width * cols),
        name="more_hidden",
    )(packed, *batches)


def prep_kernel(n_strips, n_batches, n_cuts, meta, *refs):
    strips, batches, refs = refs[:n_strips], refs[n_strips : n_strips + n_batches], refs[n_strips + n_batches :]
    turned, p_s, *hiddens, sem = refs
    width = p_s.shape[0]
    depth = width // n_cuts
    cols = turned.shape[1]
    strip = strips[0].shape[0]
    rows_of = [pl.ds(pl.multiple_of(meta[2 + n_cuts + j], 16), strip) for j in range(n_strips)]
    loads = [pltpu.make_async_copy(s, p_s.at[rows_of[j], :], sem.at[j]) for j, s in enumerate(strips)]
    for copy in loads:
        copy.start()
    for copy in loads:
        copy.wait()
    shared_units(p_s, batches, hiddens)
    for k in range(n_cuts):
        turned[k] = jnp.transpose(p_s[pl.ds(pl.multiple_of(meta[2 + k], 128), depth), 2 * cols :], (1, 0))


def shared_hidden(meta, strips, batches, width, n_cuts):
    cols = strips[0].shape[1] // 3
    rows = batches[0].shape[0]
    return pl.pallas_call(
        functools.partial(prep_kernel, len(strips), len(batches), n_cuts),
        out_shape=(pltpu.VMEM((n_cuts, cols, width // n_cuts), BF16), pltpu.VMEM((width, 3 * cols), BF16))
        + (pltpu.VMEM((rows, cols), BF16),) * len(batches),
        in_specs=[SMEM] + [ANY] * len(strips) + [VMEM] * len(batches),
        out_specs=(VMEM,) * (2 + len(batches)),
        scratch_shapes=[DMA((len(strips),))],
        compiler_params=pltpu.CompilerParams(vmem_limit_bytes=8 * MIB),
        cost_estimate=cost(8 * rows * width * cols * len(batches), 6 * width * cols),
        name="shared_hidden",
    )(meta, *strips, *batches)


def down_kernel(n_batches, part, n_cuts, meta, down, turned, *refs):
    hiddens, shareds, (kept, sent) = refs[:n_batches], refs[n_batches : 2 * n_batches], refs[2 * n_batches :]
    depth = down.shape[2] // n_cuts
    n_kept = hiddens[0].shape[0] // 2
    for i in range(n_cuts // 2):
        k = part * n_cuts // 2 + i
        place = pl.ds(pl.multiple_of(meta[2 + k], 128), depth)
        here = slice(i * depth, (i + 1) * depth)
        for n, (hidden, shared) in enumerate(zip(hiddens, shareds)):
            total = jnp.dot(hidden[...], down[0, :, place], preferred_element_type=F32)
            total = total + jnp.dot(shared[...], turned[k], preferred_element_type=F32)
            kept[n * n_kept : (n + 1) * n_kept, here] = total[:n_kept]
            sent[n * n_kept : (n + 1) * n_kept, here] = total[n_kept:].astype(BF16)


def both_down(meta, hiddens, shareds, down, turned, part, n_cuts):
    (rows, units), width = hiddens[0].shape, down.shape[2]
    rows *= len(hiddens)
    return pl.pallas_call(
        functools.partial(down_kernel, len(hiddens), part, n_cuts),
        out_shape=(pltpu.VMEM((rows // 2, width // 2), F32), pltpu.VMEM((rows // 2, width // 2), BF16)),
        in_specs=[SMEM] + [VMEM] * (2 + 2 * len(hiddens)),
        out_specs=(VMEM, VMEM),
        compiler_params=pltpu.CompilerParams(vmem_limit_bytes=6 * MIB),
        cost_estimate=cost(rows * width * (units + shareds[0].shape[1]), width * units),
        name="both_down",
    )(meta, down, turned, *hiddens, *shareds)


def local(
    tokens,
    slot,
    mask,
    hot_group,
    router_weight,
    exp_gate,
    exp_up,
    exp_down,
    sh_gate,
    sh_up,
    sh_down,
):
    n_groups, n_cuts = lax.axis_size("expert"), lax.axis_size("tensor")
    me, cut = lax.axis_index("expert"), lax.axis_index("tensor")
    rows, depth = tokens.shape
    half = rows // 2
    strip, cols = sh_gate.shape[0], sh_gate.shape[1] // n_groups
    relative = list(range(n_cuts))[::-1]
    numbers = [me, hot_group[0]] + [(cut ^ k) * depth for k in relative]
    numbers += [(me ^ j) * strip for j in range(n_groups)]
    meta = jnp.stack(numbers).astype(jnp.int32)

    features = [tokens] + [swap(tokens, "tensor", k) for k in range(1, n_cuts)]
    names = jnp.broadcast_to(slot.astype(BF16), (rows, 128))
    real = mask.astype(F32)[:, None]

    packed = jnp.concatenate(
        [
            sh_gate.reshape(strip, n_groups, cols).transpose(1, 0, 2),
            sh_up.reshape(strip, n_groups, cols).transpose(1, 0, 2),
            sh_down.reshape(n_groups, cols, strip).transpose(0, 2, 1),
        ],
        axis=2,
    )
    blocks = [lax.dynamic_index_in_dim(packed, me ^ j, 0, keepdims=False) for j in range(n_groups)]
    far_first = sorted(range(1, n_groups), key=lambda j: (-(j >> 1).bit_count(), j))
    soon, rest = far_first[: n_groups // 4], far_first[n_groups // 4 :]
    strips = {0: blocks[0]}
    strips.update({j: swap(blocks[j], "expert", j) for j in soon})

    router = router_weight.T
    names, real, meta, router, _ = tie(names, real, meta, router, blocks)
    weights = stage((router, exp_gate, exp_up, exp_down))
    halves = assemble(meta, features, names)

    routes = orders(n_groups)
    last = len(routes[0]) - 1

    def cross(pieces, phase):
        return [{j | r[phase]: swap(b, "expert", r[phase]) for j, b in p.items()} for r, p in zip(routes, pieces)]

    def join(*groups):
        return [{j: b for g in groups for j, b in g[h].items()} for h in (0, 1)]

    def with_mates(pieces):
        return join(pieces, [{j | 1: swap(b, "expert", 1) for j, b in p.items()} for p in pieces])

    own = [{0: piece} for piece in halves]
    parts = {"zero": with_mates(own)}
    came = [{}, {}]
    for phase in range(last):
        came = join(came, cross(join(own, came), phase))
    straight = cross(own, last)
    parts["one"] = with_mates(came)
    parts["two"] = with_mates(straight)
    parts["three"] = with_mates(cross(came, last))
    strips.update({j: swap(blocks[j], "expert", j) for j in rest})
    strips = [strips[j] for j in range(n_groups)]

    begun = {"late": [], "early": []}
    for name, part in parts.items():
        even = [(h, j) for h in (0, 1) for j in sorted(part[h]) if j & 1 == 0]
        many = min(len(even), ROWS // (2 * half))
        for at in range(0, len(even), many):
            stay = even[at : at + many]
            batch = [part[h][j] for h, j in stay] + [part[h][j | 1] for h, j in stay]
            done = routed_hidden(meta, batch, weights)
            begun["late" if name in ("two", "three") else "early"].append((stay, *done))

    acc = [[{}, {}], [{}, {}]]
    turned, held, *shared = shared_hidden(meta, strips, [x for _, _, x in begun["late"]], depth * n_cuts, n_cuts)
    shareds = {"late": shared}
    shareds["early"] = more_hidden(held, [x for _, _, x in begun["early"]])
    for name, some in begun.items():
        for c in (0, 1):
            kept, sent = both_down(meta, [h for _, h, _ in some], shareds[name], weights[3], turned, c, n_cuts)
            total = kept + swap(sent, "expert", 1).astype(F32)
            for i, (h, j) in enumerate(place for stay, _, _ in some for place in stay):
                acc[c][h][j] = total[i * half : (i + 1) * half]

    for phase in reversed(range(last + 1)):
        for c in (0, 1):
            away = [[j for j in a if j & r[phase]] for r, a in zip(routes, acc[c])]
            sends = [jnp.concatenate([a.pop(j) for j in js], axis=0).astype(BF16) for a, js in zip(acc[c], away)]
            came = tie(*[swap(send, "expert", r[phase]) for r, send in zip(routes, tie(*sends))])
            for r, a, js, got in zip(routes, acc[c], away, came):
                for i, j in enumerate(js):
                    a[j ^ r[phase]] = a[j ^ r[phase]] + got[i * half : (i + 1) * half].astype(F32)
    mixed = None
    for c in (0, 1):
        mine = jnp.concatenate([a[0] for a in acc[c]], axis=0)
        for i, k in enumerate(relative[c * n_cuts // 2 : (c + 1) * n_cuts // 2]):
            part = mine[:, i * depth : (i + 1) * depth]
            if k:
                part = swap(part.astype(BF16), "tensor", k).astype(F32)
            mixed = part if mixed is None else mixed + part
    return (mixed * real).astype(BF16)


def solution(mesh):
    in_specs = (
        P("expert", "tensor"),
        P("expert", None),
        P("expert"),
        P(),
        P(),
        P("expert", None, "tensor"),
        P("expert", None, "tensor"),
        P("expert", "tensor", None),
        P("expert", "tensor"),
        P("expert", "tensor"),
        P("tensor", "expert"),
    )
    out_specs = P("expert", "tensor")
    return jax.shard_map(local, mesh=mesh, in_specs=in_specs, out_specs=out_specs, check_vma=False)
```
